32 devices in a mesh: grp: 4 (over y, x), smp: 8 (over z, core).
Axes of the slice: x: 2, y: 2, z: 4, core: 2. Of those that a mesh axis runs over, the one named last changes fastest.
Arguments:
- spins_packed: int32 [32, 8192], P(None, 'smp'), may hold values from -2147483648 to 2147483646
- weight: bfloat16 [1024, 8192], P(None, 'grp'), may hold values from -0.1875 to 0.1875
- hidden_bias: float32 [8192], P('grp'), may hold values from -1.5 to 1.5
- force_w: float32 [1024, 8192], P('smp', 'grp'), may hold values from -6 to 6
- force_b: float32 [8192], P('grp'), may hold values from -6 to 6
Outputs:
- update_w: float32 [1024, 8192], P('smp', 'grp')
- update_b: float32 [8192], P('grp')
The draws below stay inside these ranges and needn't reach their ends.
All inputs are finite; a program needn't handle non-finite values.
Results may differ from the reference program's by a relative error of at most 0.0003.
Values sent between devices are 32-bit elements; how exact they have to be, the bound alone decides.
A program may use at most 64 MiB of HBM per device.

```python
import jax
import jax.numpy as jnp
from jax import lax

NV = 1024
NH = 8192
TOK_DEV = 1024
ITERS = 2
WORDS = 32
TOKENS = 8192


def with_ends(entries, stream_key, low, high):
    dims = entries.shape
    spot = [jax.random.randint(jax.random.fold_in(stream_key, axis), (), 0, dims[axis]) for axis in range(len(dims))]
    entries = entries.at[tuple(spot)].set(low)
    longest = dims.index(max(dims))
    spot[longest] = (spot[longest] + 1) % dims[longest]
    return entries.at[tuple(spot)].set(high)


def block_levels(stream_key, dims, split, smallest, top_value):
    level = 1.0
    for axis_at, shards_of in split:
        heights = jax.random.uniform(jax.random.fold_in(jax.random.fold_in(stream_key, 6), axis_at), (shards_of,), jnp.float32, smallest / len(split), top_value / len(split))
        level = level * jnp.repeat(jnp.exp(heights), dims[axis_at] // shards_of).reshape((-1,) + (1,) * (len(dims) - 1 - axis_at))
    return level


def bell_draw(rng, shape, width, reach, shards=(), kind=jnp.bfloat16):
    array = width * jax.random.normal(rng, shape, jnp.float32)
    if shards:
        array = array * block_levels(rng, shape, shards, -0.22, 0.18)
    return jnp.clip(array, -reach, reach).astype(kind)


def setup_inputs(seed: int = 0) -> dict:
    key_of = jax.random.split(jax.random.key(seed), 6)
    spins_packed = with_ends(jax.random.randint(key_of[0], (WORDS, TOKENS), -2147483648, 2147483647), jax.random.fold_in(key_of[0], 1), -2147483648, 2147483646).astype(jnp.int32)
    weight = bell_draw(key_of[1], (NV, NH), NV ** -0.5, 0.1875, ((1, 4),))
    hidden_bias = jnp.clip(jax.random.uniform(key_of[2], (NH,), jnp.float32, -1.5, 1.5) * block_levels(key_of[2], (NH,), ((0, 4),), -0.4, 0.0), -1.5, 1.5)
    force_w = bell_draw(key_of[3], (NV, NH), 1.0, 6.0, ((0, 8), (1, 4)), jnp.float32)
    force_b = bell_draw(key_of[4], (NH,), 1.0, 6.0, ((0, 4),), jnp.float32)
    return dict(spins_packed=spins_packed, weight=weight, hidden_bias=hidden_bias, force_w=force_w, force_b=force_b)


diag_shift = 0.01


def unpack(packed):
    shifts = jnp.arange(32, dtype=jnp.int32)
    bit_values = jnp.bitwise_and(jnp.right_shift(packed[:, None, :], shifts[None, :, None]), 1)
    signs = 2 * bit_values - 1
    return signs.reshape(packed.shape[0] * 32, packed.shape[1]).astype(jnp.bfloat16)


def reference(spins_packed, weight, hidden_bias, force_w, force_b):
    spins = unpack(spins_packed)
    tile_count = TOKENS // TOK_DEV
    tiles = spins.reshape(NV, tile_count, TOK_DEV).transpose(1, 0, 2)

    def activations(sample_tile):
        pre_activation = jnp.einsum("it,ih->th", sample_tile, weight, preferred_element_type=jnp.float32)
        return jnp.tanh(pre_activation + hidden_bias)

    def forward(direction_w, direction_b):
        def scan_step(running, sample_tile):
            hidden = activations(sample_tile)
            projected = jnp.einsum("it,ih->th", sample_tile, direction_w, precision=lax.Precision.HIGHEST, preferred_element_type=jnp.float32)
            return running, jnp.sum(hidden * (projected + direction_b), axis=1)

        _, sample_values = lax.scan(scan_step, jnp.zeros((), jnp.float32), tiles)
        sample_values = sample_values.reshape(TOKENS)
        return sample_values - jnp.sum(sample_values) / TOKENS

    def metric(centred, direction_w, direction_b):
        scaled = (centred / TOKENS).reshape(tile_count, TOK_DEV)

        def scan_step(running, inputs):
            sample_tile, weights_now = inputs
            hidden = activations(sample_tile)
            weighted = weights_now[:, None] * hidden
            grad_w = running[0] + jnp.einsum("it,th->ih", sample_tile, weighted, precision=lax.Precision.HIGHEST, preferred_element_type=jnp.float32)
            grad_b = running[1] + jnp.dot(weights_now, hidden, precision=lax.Precision.HIGHEST, preferred_element_type=jnp.float32)
            return (grad_w, grad_b), None

        zeros_pair = (jnp.zeros((NV, NH), jnp.float32), jnp.zeros((NH,), jnp.float32))
        (grad_w, grad_b), _ = lax.scan(scan_step, zeros_pair, (tiles, scaled))
        return grad_w + diag_shift * direction_w, grad_b + diag_shift * direction_b

    solution_w = jnp.zeros_like(force_w)
    solution_b = jnp.zeros_like(force_b)
    residual_w, residual_b = force_w, force_b
    direction_w, direction_b = force_w, force_b
    norm_now = jnp.sum(residual_w * residual_w) + jnp.sum(residual_b * residual_b)
    for iteration in range(ITERS):
        centred = forward(direction_w, direction_b)
        curvature = jnp.sum(centred * centred) / TOKENS + diag_shift * (jnp.sum(direction_w * direction_w) + jnp.sum(direction_b * direction_b))
        step_size = norm_now / curvature
        solution_w = solution_w + step_size * direction_w
        solution_b = solution_b + step_size * direction_b
        if iteration + 1 < ITERS:
            image_w, image_b = metric(centred, direction_w, direction_b)
            residual_w = residual_w - step_size * image_w
            residual_b = residual_b - step_size * image_b
            norm_next = jnp.sum(residual_w * residual_w) + jnp.sum(residual_b * residual_b)
            direction_w = residual_w + (norm_next / norm_now) * direction_w
            direction_b = residual_b + (norm_next / norm_now) * direction_b
            norm_now = norm_next
    return solution_w, solution_b
```

```python
import functools

import jax
import jax.numpy as jnp
from jax import lax
from jax.experimental import pallas as pl
from jax.experimental.pallas import tpu as pltpu
from jax.sharding import PartitionSpec as P

MESH = pl.DeviceIdType.MESH
F32, BF16 = jnp.float32, jnp.bfloat16
diag_shift = 0.01
EXTRA = 128
PAD = 16


def total(x):
    return jnp.sum(jnp.sum(x, axis=0, keepdims=True), axis=1, keepdims=True)


def kernel(
    groups, shards,
    packed_ref, weight_ref, bias_ref, force_ref, force_b_ref,
    out_ref, out_b_ref,
    packed, weight_t, bias_t, tile, spins, hidden, force_other, lhs, scaled,
    image, image_other, residual, residual_b, by_group, by_shard,
    packed_send, packed_recv, force_sem, image_send, image_recv,
    group_send, group_recv, shard_send, shard_recv,
):
    grp, smp = lax.axis_index("grp"), lax.axis_index("smp")
    chips = shards // 2
    core, chip = lax.rem(smp, 2), smp // 2
    sibling = smp + 1 - 2 * core
    words, here = packed_ref.shape
    units, rows = weight_ref.shape[1], force_ref.shape[0]
    pair = 2 * rows
    samples = chips * here
    count = samples * 2
    block = hidden_block = min(512, units)
    part = image.shape[2]
    parts = units // part

    barrier = pltpu.get_barrier_semaphore()
    for step in range(1, groups):
        pl.semaphore_signal(barrier, device_id={"grp": lax.rem(grp + step, groups)}, device_id_type=MESH)
    for step in range(1, shards):
        pl.semaphore_signal(barrier, device_id={"smp": lax.rem(smp + step, shards)}, device_id_type=MESH)
    pl.semaphore_wait(barrier, groups + shards - 2)

    packed_copies = []
    for step in range(1, chips):
        peer = lax.rem(chip + step, chips)
        packed_copies.append(
            pltpu.make_async_remote_copy(
                packed_ref, packed.at[chip], packed_send.at[step], packed_recv.at[chip],
                device_id={"smp": 2 * peer + core}, device_id_type=MESH,
            )
        )
        packed_copies[-1].start()
    force_copy = pltpu.make_async_remote_copy(
        force_ref, force_other, force_sem.at[0], force_sem.at[1],
        device_id={"smp": sibling}, device_id_type=MESH,
    )
    force_copy.start()
    packed[chip] = packed_ref[...]

    def turn(at, carry):
        cols = pl.ds(pl.multiple_of(at * 256, 256), 256)
        weight_t[cols, :] = weight_ref[:, cols].T
        bias_t[cols, :] = jnp.broadcast_to(bias_ref[:, cols], (128, 256)).T
        return carry

    lax.fori_loop(0, units // 256, turn, 0)

    def own_rows(of):
        return pl.ds(pl.multiple_of(of * rows, rows), rows)

    zero_rows = jnp.zeros((PAD - 1, units), F32)
    lhs[pl.ds(pair, PAD), :] = jnp.concatenate([force_b_ref[...] / chips, zero_rows], axis=0).astype(BF16)
    lhs[own_rows(core), :] = force_ref[...].astype(BF16)
    force_copy.wait()
    lhs[own_rows(1 - core), :] = force_other[...].astype(BF16)

    shifts = lax.broadcasted_iota(jnp.int32, (32, block), 0)
    tiles = here // block

    def values_of(cols):
        projected = jnp.dot(lhs[...], hidden[:, cols], preferred_element_type=F32)
        value = jnp.sum(projected[:pair] * spins[:, cols].astype(F32), axis=0, keepdims=True)
        return value + projected[pair : pair + 1]

    def hidden_block_of(at_chip, turn_at, carry):
        local = pl.ds(pl.multiple_of(turn_at * block, block), block)
        cols = pl.ds(pl.multiple_of(at_chip * here + turn_at * block, block), block)
        for word in range(words):
            bits = jnp.right_shift(jnp.broadcast_to(packed[at_chip, word : word + 1, local], (32, block)), shifts)
            tile[word * 32 : word * 32 + 32, :] = (2 * jnp.bitwise_and(bits, 1) - 1).astype(F32).astype(BF16)
        spins[:, cols] = tile[pl.ds(pl.multiple_of(chip * pair, pair), pair), :]
        for unit in range(0, units, hidden_block):
            these = pl.ds(unit, hidden_block)
            pre = jnp.dot(weight_t[these, :], tile[...], preferred_element_type=F32)
            bias = bias_t[these, :]
            pre = pre + jnp.concatenate([bias] * (block // 128), axis=1)
            hidden[these, cols] = jnp.tanh(pre).astype(BF16)
        by_group[0, grp, :, cols] = values_of(cols)
        return carry

    for step in range(chips):
        at_chip = lax.rem(chip + chips - step, chips)
        if step:
            pltpu.make_async_remote_copy(
                packed_ref, packed.at[at_chip], packed_send.at[step], packed_recv.at[at_chip],
                device_id={"smp": sibling}, device_id_type=MESH,
            ).wait_recv()
        lax.fori_loop(0, tiles, functools.partial(hidden_block_of, at_chip), 0)
    for copy in packed_copies:
        copy.wait_send()

    def gather(slots, which, axis, size, me, send, recv):
        copies = []
        for step in range(1, size):
            copies.append(
                pltpu.make_async_remote_copy(
                    slots.at[which, me], slots.at[which, me], send.at[which, step], recv.at[which, me],
                    device_id={axis: lax.rem(me + step, size)}, device_id_type=MESH,
                )
            )
            copies[-1].start()
        for step in range(1, size):
            source = lax.rem(me + size - step, size)
            pltpu.make_async_remote_copy(
                slots.at[which, source], slots.at[which, source], send.at[which, step], recv.at[which, source],
                device_id={axis: source}, device_id_type=MESH,
            ).wait_recv()
        for copy in copies:
            copy.wait_send()

    lane = lax.broadcasted_iota(jnp.int32, (1, EXTRA), 1)

    def reduce_values(which, first, second):
        by_group[which, grp, :, samples:] = jnp.where(lane == 0, first, jnp.where(lane == 1, second, 0.0))
        gather(by_group, which, "grp", groups, grp, group_send, group_recv)
        mine = by_group[which, 0]
        for source in range(1, groups):
            mine = mine + by_group[which, source]
        by_shard[which, smp] = mine
        gather(by_shard, which, "smp", shards, smp, shard_send, shard_recv)
        halves = []
        for half in range(2):
            value = by_shard[which, half]
            for source in range(half + 2, shards, 2):
                value = value + by_shard[which, source]
            halves.append(value)
        extra = halves[0][:, samples:] + halves[1][:, samples:]
        first = jnp.sum(jnp.where(lane == 0, extra, 0.0), axis=1, keepdims=True)
        second = jnp.sum(jnp.where(lane == 1, extra, 0.0), axis=1, keepdims=True)
        return halves[0][:, :samples], halves[1][:, :samples], first, second

    def centre(low, high):
        mean = total(low) / count + total(high) / count
        return low - mean, high - mean

    force_dot = total(force_ref[...] * force_ref[...]) + total(force_b_ref[...] * force_b_ref[...]) / shards
    low0, high0, norm0, _ = reduce_values(0, force_dot, jnp.zeros((1, 1), F32))
    low, high = centre(low0, high0)
    curvature0 = total(low * low) / count + total(high * high) / count + diag_shift * norm0
    step0 = norm0 / curvature0

    mine = (jnp.where(core == 0, low, high)).astype(F32)
    for at in range(0, samples, block):
        weights = mine[:, at : at + block]
        scaled[:pair, at : at + block] = (spins[:, at : at + block].astype(F32) * weights).astype(BF16)
        scaled[pair:, at : at + block] = jnp.concatenate(
            [weights, jnp.zeros((PAD - 1, block), F32)], axis=0
        ).astype(BF16)

    def image_copy(at):
        return pltpu.make_async_remote_copy(
            image.at[at], image_other.at[at], image_send.at[at], image_recv.at[at],
            device_id={"smp": sibling}, device_id_type=MESH,
        )

    def image_part(at, carry):
        these = pl.ds(pl.multiple_of(at * part, part), part)
        image[at] = lax.dot_general(
            scaled[...], hidden[these, :], (((1,), (1,)), ((), ())), preferred_element_type=F32
        )
        image_copy(at).start()
        return carry

    lax.fori_loop(0, parts, image_part, 0)

    scale = 1.0 / count

    def residual_part(at, carry):
        first, second = carry
        these = pl.ds(pl.multiple_of(at * part, part), part)
        image_copy(at).wait()

        def next_residual(which, force):
            whole = image[at, which, :] + image_other[at, which, :]
            return force - step0 * (whole * scale + diag_shift * force)

        own = next_residual(own_rows(core), force_ref[:, these])
        residual[:, these] = own
        lhs[own_rows(core), these] = own.astype(BF16)
        lhs[own_rows(1 - core), these] = next_residual(own_rows(1 - core), force_other[:, these]).astype(BF16)
        own_b = next_residual(pl.ds(pair, 1), force_b_ref[:, these])
        residual_b[:, these] = own_b
        lhs[pl.ds(pair, PAD), these] = jnp.concatenate([own_b / chips, jnp.zeros((PAD - 1, part), F32)], axis=0).astype(BF16)
        first = first + total(own * own) + total(own_b * own_b) / shards
        second = second + total(own * force_ref[:, these]) + total(own_b * force_b_ref[:, these]) / shards
        return first, second

    zero = jnp.zeros((1, 1), F32)
    own_norm, own_cross = lax.fori_loop(0, parts, residual_part, (zero, zero))

    def second_values(at, carry):
        cols = pl.ds(pl.multiple_of(at * block, block), block)
        by_group[1, grp, :, cols] = values_of(cols)
        return carry

    lax.fori_loop(0, samples // block, second_values, 0)
    low1, high1, norm1, cross = reduce_values(1, own_norm, own_cross)
    beta = norm1 / norm0
    low, high = centre(low1 + beta * low0, high1 + beta * high0)
    direction_dot = norm1 + 2.0 * beta * cross + beta * beta * norm0
    curvature1 = total(low * low) / count + total(high * high) / count + diag_shift * direction_dot
    step1 = norm1 / curvature1

    out_ref[...] = step0 * force_ref[...] + step1 * (residual[...] + beta * force_ref[...])
    out_b_ref[...] = step0 * force_b_ref[...] + step1 * (residual_b[...] + beta * force_b_ref[...])


def body(groups, shards, spins_packed, weight, hidden_bias, force_w, force_b):
    words, here = spins_packed.shape
    inputs, units = weight.shape
    rows = force_w.shape[0]
    chips = shards // 2
    samples, pair = chips * here, 2 * rows
    part = 256
    parts = units // part
    vmem = pl.BlockSpec(memory_space=pltpu.VMEM)
    dma = pltpu.SemaphoreType.DMA
    update_w, update_b = pl.pallas_call(
        functools.partial(kernel, groups, shards),
        out_shape=(jax.ShapeDtypeStruct((rows, units), F32), jax.ShapeDtypeStruct((1, units), F32)),
        in_specs=[vmem] * 5,
        out_specs=(vmem, vmem),
        scratch_shapes=[
            pltpu.VMEM((chips, words, here), jnp.int32),
            pltpu.VMEM((units, inputs), BF16),
            pltpu.VMEM((units, 128), F32),
            pltpu.VMEM((inputs, min(512, units)), BF16),
            pltpu.VMEM((pair, samples), BF16),
            pltpu.VMEM((units, samples), BF16),
            pltpu.VMEM((rows, units), F32),
            pltpu.VMEM((pair + PAD, units), BF16),
            pltpu.VMEM((pair + PAD, samples), BF16),
            pltpu.VMEM((parts, pair + PAD, part), F32),
            pltpu.VMEM((parts, pair + PAD, part), F32),
            pltpu.VMEM((rows, units), F32),
            pltpu.VMEM((1, units), F32),
            pltpu.VMEM((2, groups, 1, samples + EXTRA), F32),
            pltpu.VMEM((2, shards, 1, samples + EXTRA), F32),
            dma((chips,)),
            dma((chips,)),
            dma((2,)),
            dma((parts,)),
            dma((parts,)),
            dma((2, groups)),
            dma((2, groups)),
            dma((2, shards)),
            dma((2, shards)),
        ],
        compiler_params=pltpu.CompilerParams(
            collective_id=0, has_side_effects=True, vmem_limit_bytes=62 * 1024 * 1024
        ),
    )(spins_packed, weight, hidden_bias.reshape(1, -1), force_w, force_b.reshape(1, -1))
    return update_w, update_b.reshape(-1)


def solution(mesh):
    placed = (P(None, "smp"), P(None, "grp"), P("grp"), P("smp", "grp"), P("grp"))
    return jax.shard_map(
        functools.partial(body, mesh.shape["grp"], mesh.shape["smp"]),
        mesh=mesh, in_specs=placed, out_specs=(P("smp", "grp"), P("grp")), check_vma=False,
    )
```
